32 devices in a mesh: tensor: 2 (over x), context: 8 (over z, core), dp: 2 (over y).
Axes of the slice: x: 2, y: 2, z: 4, core: 2. Of those that a mesh axis runs over, the one named last changes fastest.
Arguments:
- query_a: bfloat16 [2048, 1024], P(('dp', 'context'), 'tensor'), parts along dimension 0, may hold values from -5 to 5
- key_a: bfloat16 [2048, 256], P(('dp', 'context'), 'tensor'), parts along dimension 0, may hold values from -5 to 5
- value_a: bfloat16 [2048, 256], P(('dp', 'context'), 'tensor'), parts along dimension 0, may hold values from -12 to 12
- grad_out_a: bfloat16 [2048, 1024], P(('dp', 'context'), 'tensor'), parts along dimension 0, may hold values from -6 to 6
- query_b: bfloat16 [2048, 1024], P(('dp', 'context'), 'tensor'), parts along dimension 0, may hold values from -5 to 5
- key_b: bfloat16 [2048, 256], P(('dp', 'context'), 'tensor'), parts along dimension 0, may hold values from -5 to 5
- value_b: bfloat16 [2048, 256], P(('dp', 'context'), 'tensor'), parts along dimension 0, may hold values from -12 to 12
- slab_owner: int32 [8], replicated, may hold values from 0 to 7, each once
Outputs:
- out_b: bfloat16 [2048, 1024], P(('dp', 'context'), 'tensor'), parts along dimension 0
- grad_query_a: bfloat16 [2048, 1024], P(('dp', 'context'), 'tensor'), parts along dimension 0
- grad_key_a: bfloat16 [2048, 256], P(('dp', 'context'), 'tensor'), parts along dimension 0
- grad_value_a: bfloat16 [2048, 256], P(('dp', 'context'), 'tensor'), parts along dimension 0
The draws below stay inside these ranges and needn't reach their ends.
There are 2 independent parts, one for each index of `dp`. The reference program is written for one: setup_inputs(seed, part) draws one part's arguments, and reference() takes and returns one part's arrays. A program takes and returns all parts, laid end to end along the dimension named above; an argument that names none is the same for every part. Nothing has to cross between parts.
Inputs may be any that keep to these rules, and one draw needn't show every extreme that they name: `slab_owner`: each number appears once.
All inputs are finite; a program needn't handle non-finite values.
Results may differ from the reference program's by a relative error of at most 0.0091.
Values may be sent and summed in bfloat16 or wider, within the bound.
A program may use at most 64 MiB of HBM per device.

```python
import jax
import jax.numpy as jnp
from jax import lax

HEAD_DIM = 128
HEADS_DEV = 4
TOK_DEV = 128
HEADS = 8
KV_HEADS = 2
TOKENS = 1024
N_CONTEXT = 8


def random_base(key, label, width):
    inner = jax.random.fold_in(key, label)
    return jnp.clip(1.4 * jax.random.normal(inner, (TOKENS, width), jnp.float32), -5.0, 5.0)


def drawn_queries(key, label):
    values = random_base(key, label + 1, HEADS * HEAD_DIM)
    return values.astype(jnp.bfloat16)


def drawn_keys(key, label):
    values = random_base(key, label + 7, KV_HEADS * HEAD_DIM)
    return values.astype(jnp.bfloat16)


def draw_query_a(key, part):
    return drawn_queries(key, 101)


def draw_key_a(key, part):
    return drawn_keys(key, 101)


def draw_query_b(key, part):
    return drawn_queries(key, 202)


def draw_key_b(key, part):
    return drawn_keys(key, 202)


def steps_of(stream_key, dims, cuts, low, top_value):
    level, own = 1.0, jax.random.fold_in(stream_key, 6)
    for position, shards_of in cuts:
        steps = jnp.exp(jax.random.uniform(jax.random.fold_in(own, position), (shards_of,), jnp.float32, low / len(cuts), top_value / len(cuts)))
        level = level * jnp.repeat(steps, dims[position] // shards_of).reshape([-1 if axis == position else 1 for axis in range(len(dims))])
    return level


def bell_draw(own_key, shape, spread, reach, pieces=(), held_as=jnp.bfloat16):
    drawn = jax.random.normal(own_key, shape, jnp.float32) * spread
    if len(pieces) > 0:
        drawn = steps_of(own_key, shape, pieces, -0.22, 0.18) * drawn
    return jnp.clip(drawn, min=-reach, max=reach).astype(held_as)


def setup_inputs(seed: int = 0, part: int = 0) -> dict:
    key_of = jax.random.split(jax.random.key(seed), 9)
    own_keys = jax.random.split(jax.random.fold_in(key_of[8], part), 9)
    query_a = draw_query_a(jax.random.fold_in(jax.random.fold_in(key_of[8], part), 71), part)
    key_a = draw_key_a(jax.random.fold_in(jax.random.fold_in(key_of[8], part), 71), part)
    value_a = bell_draw(own_keys[2], (TOKENS, KV_HEADS * HEAD_DIM), 2.0, 12.0, ((0, 8), (1, 2)))
    grad_out_a = bell_draw(own_keys[3], (TOKENS, HEADS * HEAD_DIM), 1.0, 6.0, ((0, 8), (1, 2)))
    query_b = draw_query_b(jax.random.fold_in(jax.random.fold_in(key_of[8], part), 71), part)
    key_b = draw_key_b(jax.random.fold_in(jax.random.fold_in(key_of[8], part), 71), part)
    value_b = bell_draw(own_keys[6], (TOKENS, KV_HEADS * HEAD_DIM), 2.0, 12.0, ((0, 8), (1, 2)))
    slab_owner = jax.random.permutation(key_of[7], N_CONTEXT).astype(jnp.int32)
    return {"query_a": query_a, "key_a": key_a, "value_a": value_a, "grad_out_a": grad_out_a, "query_b": query_b, "key_b": key_b, "value_b": value_b, "slab_owner": slab_owner}


def slab_places(slab_owner):
    half = TOK_DEV // 2
    rows = jnp.arange(TOKENS, dtype=jnp.int32)
    holder = rows // TOK_DEV
    within = rows % TOK_DEV
    owner_slab = slab_owner[holder].astype(jnp.int32)
    slab = jnp.where(within < half, owner_slab, 2 * N_CONTEXT - 1 - owner_slab)
    return (slab * half + within % half).astype(jnp.int32)


def scores_of(queries, keys, query_places, places):
    raw = jnp.einsum("bhd,nd->hbn", queries.astype(jnp.float32), keys.astype(jnp.float32))
    allowed = places[None, None, :] <= query_places[None, :, None]
    return raw * HEAD_DIM ** -0.5, allowed


def forward_rows(queries, query_places, keys, values, places):
    scaled, allowed = scores_of(queries, keys, query_places, places)
    top = jnp.max(jnp.where(allowed, scaled, -jnp.inf), axis=2)
    raised = jnp.where(allowed, jnp.exp(scaled - top[:, :, None]), 0.0)
    total = jnp.sum(raised, axis=2)
    weights = lax.optimization_barrier(raised.astype(jnp.bfloat16))
    summed = jnp.einsum("hbn,nd->bhd", weights.astype(jnp.float32), values.astype(jnp.float32))
    mixed = summed / jnp.transpose(total)[:, :, None]
    return mixed, jnp.transpose(top + jnp.log(total))


def forward_all(queries, keys, values, places):
    query_rows = min(512, TOKENS)
    blocks = TOKENS // query_rows

    def one_block(item):
        return forward_rows(item[0], item[1], keys, values, places)

    mixed, log_total = lax.map(one_block, (queries.reshape(blocks, query_rows, HEADS_DEV, HEAD_DIM), places.reshape(blocks, query_rows)))
    return mixed.reshape(TOKENS, HEADS_DEV, HEAD_DIM), log_total.reshape(TOKENS, HEADS_DEV)


def backward_all(queries, keys, values, grads, places):
    mixed, log_total = forward_all(queries, keys, values, places)
    delta = jnp.sum(grads.astype(jnp.float32) * mixed, axis=2)
    query_rows = min(512, TOKENS)
    blocks = TOKENS // query_rows
    scale = HEAD_DIM ** -0.5

    def advance(carried, item):
        block_query, block_grad, block_places, block_log, block_delta = item
        scaled, allowed = scores_of(block_query, keys, block_places, places)
        prob = jnp.where(allowed, jnp.exp(scaled - jnp.transpose(block_log)[:, :, None]), 0.0)
        prob_grad = jnp.einsum("bhd,nd->hbn", block_grad.astype(jnp.float32), values.astype(jnp.float32))
        score_grad = (prob * (prob_grad - jnp.transpose(block_delta)[:, :, None])).astype(jnp.bfloat16)
        low_prob = prob.astype(jnp.bfloat16)
        score_grad, low_prob = lax.optimization_barrier((score_grad, low_prob))
        query_grad = jnp.einsum("hbn,nd->bhd", score_grad.astype(jnp.float32), keys.astype(jnp.float32)) * scale
        key_sum = carried[0] + jnp.einsum("hbn,bhd->nd", score_grad.astype(jnp.float32), block_query.astype(jnp.float32))
        value_sum = carried[1] + jnp.einsum("hbn,bhd->nd", low_prob.astype(jnp.float32), block_grad.astype(jnp.float32))
        return (key_sum, value_sum), query_grad.astype(jnp.bfloat16)

    items = (queries.reshape(blocks, query_rows, HEADS_DEV, HEAD_DIM), grads.reshape(blocks, query_rows, HEADS_DEV, HEAD_DIM), places.reshape(blocks, query_rows), log_total.reshape(blocks, query_rows, HEADS_DEV), delta.reshape(blocks, query_rows, HEADS_DEV))
    empty = jnp.zeros((TOKENS, HEAD_DIM), jnp.float32)
    sums, query_grad = lax.scan(advance, (empty, empty), items)
    key_grad = (sums[0] * scale).astype(jnp.bfloat16)
    value_grad = sums[1].astype(jnp.bfloat16)
    return query_grad.reshape(TOKENS, HEADS_DEV * HEAD_DIM), key_grad, value_grad


def reference(query_a, key_a, value_a, grad_out_a, query_b, key_b, value_b, slab_owner):
    places = slab_places(slab_owner)
    width = HEADS_DEV * HEAD_DIM
    outs_b = []
    grads_query = []
    grads_key = []
    grads_value = []
    for group in range(KV_HEADS):
        head_lo = group * width
        kv_lo = group * HEAD_DIM
        group_query_b = query_b[:, head_lo:head_lo + width].reshape(TOKENS, HEADS_DEV, HEAD_DIM)
        mixed_b, unused = forward_all(group_query_b, key_b[:, kv_lo:kv_lo + HEAD_DIM], value_b[:, kv_lo:kv_lo + HEAD_DIM], places)
        outs_b.append(mixed_b.reshape(TOKENS, width).astype(jnp.bfloat16))
        group_query_a = query_a[:, head_lo:head_lo + width].reshape(TOKENS, HEADS_DEV, HEAD_DIM)
        group_grad = grad_out_a[:, head_lo:head_lo + width].reshape(TOKENS, HEADS_DEV, HEAD_DIM)
        query_grad, key_grad, value_grad = backward_all(group_query_a, key_a[:, kv_lo:kv_lo + HEAD_DIM], value_a[:, kv_lo:kv_lo + HEAD_DIM], group_grad, places)
        grads_query.append(query_grad)
        grads_key.append(key_grad)
        grads_value.append(value_grad)
    return (jnp.concatenate(outs_b, axis=1), jnp.concatenate(grads_query, axis=1), jnp.concatenate(grads_key, axis=1), jnp.concatenate(grads_value, axis=1))
```

```python
import functools

import jax
import jax.numpy as jnp
from jax import lax
from jax.experimental import pallas as pl
from jax.experimental.pallas import tpu as pltpu
from jax.sharding import PartitionSpec as P

LOW = -1e30
LOG2E = 1.4426950408889634
F32 = jnp.float32
BF16 = jnp.bfloat16


def dot_nt(a, b):
    return lax.dot_general(a, b, (((1,), (1,)), ((), ())), preferred_element_type=F32)


def dot_nn(a, b):
    return lax.dot_general(a, b, (((1,), (0,)), ((), ())), preferred_element_type=F32)


def dot_tn(a, b):
    return lax.dot_general(a, b, (((0,), (0,)), ((), ())), preferred_element_type=F32)


def groups(x, op):
    out = x[0:8]
    for i in range(8, x.shape[0], 8):
        out = op(out, x[i:i + 8])
    return out


def kernel(
    n, tok, heads, dim,
    owner, qa, ka, va, ga, qb, kb, vb,
    out_b, out_dq, out_dk, out_dv,
    kv, q_a, g_a, q_b, scores, pgrad, top, tot, dsum, acc_t, res_q, res_b, res_kv,
    own, pair_out, pair_in, far_out, far_in,
    load_sem, store_sem, recv_sem, right_sem, left_sem, mate_sem,
    pair_send, pair_recv, far_send, far_recv,
):
    chips = n // 2
    me = lax.axis_index("context")
    chip, core = me // 2, me % 2
    mate = chip * 2 + (1 - core)
    rows = heads * tok
    half = tok // 2
    scale = dim ** (-0.5)
    factor = scale * LOG2E

    def to(idx):
        return dict(device_id={"context": idx}, device_id_type=pl.DeviceIdType.MESH)

    def kv_load(b, j):
        src = ((ka, va), (kb, vb))[b][j]
        return pltpu.make_async_copy(src, kv.at[b, me, j], load_sem.at[b * 2 + j])

    def head_load(i, h):
        src, dst = ((qa, q_a), (ga, g_a), (qb, q_b))[i]
        return pltpu.make_async_copy(
            src.at[:, pl.ds(h * dim, dim)], dst.at[pl.ds(h * tok, tok), :],
            load_sem.at[4 + i * heads + h],
        )

    for b in range(2):
        for j in range(2):
            kv_load(b, j).start()
    for i in range(3):
        for h in range(heads):
            head_load(i, h).start()

    barrier = pltpu.get_barrier_semaphore()
    for off in range(1, chips):
        pl.semaphore_signal(barrier, inc=1, **to(lax.rem(chip + off, chips) * 2 + core))
    pl.semaphore_signal(barrier, inc=1, **to(mate))
    for b in range(2):
        for j in range(2):
            kv_load(b, j).wait()
    pl.semaphore_wait(barrier, chips)

    def hop(b, slot, j, target, sems):
        return pltpu.make_async_remote_copy(
            src_ref=kv.at[b, slot, j], dst_ref=kv.at[b, slot, j],
            send_sem=sems.at[b, slot, j], recv_sem=recv_sem.at[b, slot, j], **to(target),
        )

    def go_right(b, slot, j):
        return hop(b, slot, j, jnp.minimum(me + 2, n - 1), right_sem)

    def go_left(b, slot, j):
        return hop(b, slot, j, jnp.maximum(me - 2, 0), left_sem)

    def go_mate(b, slot, j):
        return hop(b, slot, j, mate, mate_sem)

    can_right = chip + 1 < chips
    can_left = chip > 0

    def spread_own(b):
        @pl.when(can_right)
        def _():
            for j in range(2):
                go_right(b, me, j).start()

        @pl.when(can_left)
        def _():
            for j in range(2):
                go_left(b, me, j).start()

        for j in range(2):
            go_mate(b, me, j).start()

    def relay(b, t):
        from_left = me - 2 * t
        from_right = me + 2 * t
        for j in range(2):
            @pl.when(chip - t >= 0)
            def _():
                slot = jnp.maximum(from_left, 0)
                hop(b, slot, j, mate, mate_sem).wait_recv()

                @pl.when(can_right)
                def _():
                    go_right(b, slot, j).start()
                go_mate(b, slot, j).start()

            @pl.when(chip + t < chips)
            def _():
                slot = jnp.minimum(from_right, n - 1)
                hop(b, slot, j, mate, mate_sem).wait_recv()

                @pl.when(can_left)
                def _():
                    go_left(b, slot, j).start()
                go_mate(b, slot, j).start()

    def take_mate(b, slot):
        for j in range(2):
            hop(b, slot, j, mate, mate_sem).wait_recv()

    spread_own(0)

    lane = lax.broadcasted_iota(jnp.int32, (1, rows), 1) % tok
    mine = owner[me]
    places = jnp.where(lane < half, mine * half + lane, (2 * n - 1 - mine) * half + lane - half)
    key_row = lax.broadcasted_iota(jnp.int32, (half, rows), 0)

    def masked(s, slot):
        o = owner[slot]
        first = jnp.where(key_row <= places - o * half, s[:half], LOW)
        second = jnp.where(key_row <= places - (2 * n - 1 - o) * half, s[half:], LOW)
        return first, second

    def score_block(b, slot, queries):
        first, second = masked(dot_nt(kv[b, slot, 0], queries[...]), slot)
        scores[slot, :half] = first
        scores[slot, half:] = second
        top[...] = jnp.maximum(
            top[...], jnp.maximum(groups(first, jnp.maximum), groups(second, jnp.maximum))
        )

    def first_a(slot):
        score_block(0, slot, q_a)
        pgrad[slot] = dot_nt(kv[0, slot, 1], g_a[...])

    for i in range(3):
        for h in range(heads):
            head_load(i, h).wait()
    top[...] = jnp.full_like(top, LOW)
    first_a(me)

    def gather_a(t, _):
        relay(0, t)

        @pl.when(chip - t >= 0)
        def _():
            first_a(jnp.maximum(me - 2 * t, 0))

        @pl.when(chip + t < chips)
        def _():
            first_a(jnp.minimum(me + 2 * t, n - 1))
        return 0

    lax.fori_loop(1, chips, gather_a, 0)
    spread_own(1)

    def mates_a(d, _):
        slot = 2 * d + 1 - core
        take_mate(0, slot)
        first_a(slot)
        return 0

    lax.fori_loop(0, chips, mates_a, 0)

    peak = jnp.max(top[...], axis=0, keepdims=True) * factor
    tot[...] = jnp.zeros_like(tot)
    dsum[...] = jnp.zeros_like(dsum)

    def second_a(i, _):
        p = jnp.exp2(scores[i] * factor - peak)
        scores[i] = p
        tot[...] += groups(p, jnp.add)
        dsum[...] += groups(p * pgrad[i], jnp.add)
        return 0

    lax.fori_loop(0, n, second_a, 0)
    inv = 1.0 / jnp.sum(tot[...], axis=0, keepdims=True)
    delta = jnp.sum(dsum[...], axis=0, keepdims=True) * inv
    acc_t[...] = jnp.zeros_like(acc_t)

    def grads(slot):
        prob = scores[slot] * inv
        sg = (prob * (pgrad[slot] - delta)).astype(BF16)
        dk = dot_nn(sg, q_a[...])
        dv = dot_nn(prob.astype(BF16), g_a[...])
        acc_t[...] += dot_tn(kv[0, slot, 0], sg)
        return dk, dv

    def pair(d):
        return pltpu.make_async_remote_copy(
            src_ref=pair_out.at[d], dst_ref=pair_in.at[d],
            send_sem=pair_send.at[d], recv_sem=pair_recv.at[d], **to(mate),
        )

    def far(d):
        return pltpu.make_async_remote_copy(
            src_ref=far_out.at[d], dst_ref=far_in.at[chip],
            send_sem=far_send.at[d], recv_sem=far_recv.at[chip], **to(d * 2 + core),
        )

    def ship(d):
        pair(d).wait_recv()
        far_out[d] = (own[d] + pair_in[d].astype(F32)).astype(BF16)
        far(d).start()

    def third_a(t, _):
        @pl.when(t >= 1)
        def _():
            relay(1, t)
        d = lax.rem(chip + t + 1, chips)
        dk, dv = grads(2 * d + 1 - core)
        pair_out[d, 0] = dk.astype(BF16)
        pair_out[d, 1] = dv.astype(BF16)
        pair(d).start()
        dk, dv = grads(2 * d + core)
        own[d, 0] = dk
        own[d, 1] = dv

        @pl.when(t >= 1)
        def _():
            ship(lax.rem(chip + t, chips))
        return 0

    lax.fori_loop(0, chips, third_a, 0)

    def out_copy(i, h):
        src, dst = ((res_q, out_dq), (res_b, out_b))[i]
        return pltpu.make_async_copy(
            src.at[pl.ds(h * tok, tok), :], dst.at[:, pl.ds(h * dim, dim)],
            store_sem.at[i * heads + h],
        )

    res_q[...] = jnp.transpose(acc_t[...] * scale).astype(BF16)
    for h in range(heads):
        out_copy(0, h).start()

    top[...] = jnp.full_like(top, LOW)

    def take_b(d, _):
        take_mate(1, 2 * d + 1 - core)
        return 0

    lax.fori_loop(0, chips, take_b, 0)

    def first_b(i, _):
        score_block(1, i, q_b)
        return 0

    lax.fori_loop(0, n, first_b, 0)
    peak_b = jnp.max(top[...], axis=0, keepdims=True) * factor
    tot[...] = jnp.zeros_like(tot)
    acc_t[...] = jnp.zeros_like(acc_t)

    def second_b(i, _):
        p = jnp.exp2(scores[i] * factor - peak_b)
        tot[...] += groups(p, jnp.add)
        acc_t[...] += dot_tn(kv[1, i, 1], p.astype(BF16))
        return 0

    lax.fori_loop(0, n, second_b, 0)
    total_b = jnp.sum(tot[...], axis=0, keepdims=True)
    res_b[...] = jnp.transpose(acc_t[...] / total_b).astype(BF16)
    for h in range(heads):
        out_copy(1, h).start()

    pair(chip).wait_recv()
    own[chip] = own[chip] + pair_in[chip].astype(F32)

    def gather_sum(off, _):
        d = lax.rem(chip + off, chips)
        pltpu.make_async_remote_copy(
            src_ref=far_out.at[d], dst_ref=far_in.at[d],
            send_sem=far_send.at[d], recv_sem=far_recv.at[d], **to(d * 2 + core),
        ).wait_recv()
        own[chip] = own[chip] + far_in[d].astype(F32)
        return 0

    lax.fori_loop(1, chips, gather_sum, 0)
    res_kv[0] = (own[chip, 0] * scale).astype(BF16)
    res_kv[1] = own[chip, 1].astype(BF16)
    kv_out = [
        pltpu.make_async_copy(res_kv.at[j], (out_dk, out_dv)[j], store_sem.at[2 * heads + j])
        for j in range(2)
    ]
    for j in range(2):
        kv_out[j].start()

    def drain_far(off, _):
        far(lax.rem(chip + off, chips)).wait_send()
        return 0

    lax.fori_loop(1, chips, drain_far, 0)

    def drain(d, _):
        pair(d).wait_send()
        slot = 2 * d + core
        for b in range(2):
            for j in range(2):
                go_mate(b, slot, j).wait_send()

                @pl.when(jnp.logical_and(can_right, d <= chip))
                def _():
                    go_right(b, slot, j).wait_send()

                @pl.when(jnp.logical_and(can_left, d >= chip))
                def _():
                    go_left(b, slot, j).wait_send()
        return 0

    lax.fori_loop(0, chips, drain, 0)
    for i in range(2):
        for h in range(heads):
            out_copy(i, h).wait()
    for j in range(2):
        kv_out[j].wait()


def on_device(n, qa, ka, va, ga, qb, kb, vb, owner):
    tok, dim = ka.shape
    heads = qa.shape[1] // dim
    rows = heads * tok
    chips = n // 2
    any_spec = pl.BlockSpec(memory_space=pl.ANY)
    sem = pltpu.SemaphoreType.DMA
    return pl.pallas_call(
        functools.partial(kernel, n, tok, heads, dim),
        out_shape=(
            jax.ShapeDtypeStruct(qb.shape, BF16),
            jax.ShapeDtypeStruct(qa.shape, BF16),
            jax.ShapeDtypeStruct(ka.shape, BF16),
            jax.ShapeDtypeStruct(va.shape, BF16),
        ),
        in_specs=[pl.BlockSpec(memory_space=pltpu.SMEM)] + [any_spec] * 7,
        out_specs=(any_spec,) * 4,
        scratch_shapes=[
            pltpu.VMEM((2, n, 2, tok, dim), BF16),
            pltpu.VMEM((rows, dim), BF16),
            pltpu.VMEM((rows, dim), BF16),
            pltpu.VMEM((rows, dim), BF16),
            pltpu.VMEM((n, tok, rows), F32),
            pltpu.VMEM((n, tok, rows), F32),
            pltpu.VMEM((8, rows), F32),
            pltpu.VMEM((8, rows), F32),
            pltpu.VMEM((8, rows), F32),
            pltpu.VMEM((dim, rows), F32),
            pltpu.VMEM((rows, dim), BF16),
            pltpu.VMEM((rows, dim), BF16),
            pltpu.VMEM((2, tok, dim), BF16),
            pltpu.VMEM((chips, 2, tok, dim), F32),
            pltpu.VMEM((chips, 2, tok, dim), BF16),
            pltpu.VMEM((chips, 2, tok, dim), BF16),
            pltpu.VMEM((chips, 2, tok, dim), BF16),
            pltpu.VMEM((chips, 2, tok, dim), BF16),
            sem((4 + 3 * heads,)),
            sem((2 * heads + 2,)),
            sem((2, n, 2)),
            sem((2, n, 2)),
            sem((2, n, 2)),
            sem((2, n, 2)),
            sem((chips,)),
            sem((chips,)),
            sem((chips,)),
            sem((chips,)),
        ],
        compiler_params=pltpu.CompilerParams(collective_id=0, has_side_effects=True),
    )(owner, qa, ka, va, ga, qb, kb, vb)


def solution(mesh):
    spec = P(("dp", "context"), "tensor")
    return jax.shard_map(
        functools.partial(on_device, mesh.shape["context"]),
        mesh=mesh,
        in_specs=(spec,) * 7 + (P(),),
        out_specs=(spec,) * 4,
        check_vma=False,
    )
```

```python
import functools

import jax
import jax.numpy as jnp
from jax import lax
from jax.experimental import pallas as pl
from jax.experimental.pallas import tpu as pltpu
from jax.sharding import PartitionSpec as P

LOW = -1e30
LOG2E = 1.4426950408889634
F32 = jnp.float32
BF16 = jnp.bfloat16


def dot_nt(a, b):
    return lax.dot_general(a, b, (((1,), (1,)), ((), ())), preferred_element_type=F32)


def dot_nn(a, b):
    return lax.dot_general(a, b, (((1,), (0,)), ((), ())), preferred_element_type=F32)


def dot_tn(a, b):
    return lax.dot_general(a, b, (((0,), (0,)), ((), ())), preferred_element_type=F32)


def groups(x, op):
    out = x[0:8]
    for i in range(8, x.shape[0], 8):
        out = op(out, x[i:i + 8])
    return out


def kernel(
    n, tok, heads, dim,
    owner, qa, ka, va, ga, qb, kb, vb,
    out_b, out_dq, out_dk, out_dv,
    kv, q_a, g_a, q_b, scores, pgrad, top, tot, dsum, acc_t, both,
    own, pair_out, pair_in, far_out, far_in,
    load_sem, recv_sem, right_sem, left_sem, mate_sem,
    pair_send, pair_recv, far_send, far_recv,
):
    chips = n // 2
    me = lax.axis_index("context")
    chip, core = me // 2, me % 2
    mate = chip * 2 + (1 - core)
    rows = heads * tok
    half = tok // 2
    scale = dim ** (-0.5)
    factor = scale * LOG2E

    def to(idx):
        return dict(device_id={"context": idx}, device_id_type=pl.DeviceIdType.MESH)

    def kv_load(b, j):
        src = ((ka, va), (kb, vb))[b][j]
        return pltpu.make_async_copy(src, kv.at[b, me, j], load_sem.at[b * 2 + j])

    def head_load(i, h):
        src, dst = ((qa, q_a), (ga, g_a), (qb, q_b))[i]
        return pltpu.make_async_copy(
            src.at[:, pl.ds(h * dim, dim)], dst.at[pl.ds(h * tok, tok), :],
            load_sem.at[4 + i * heads + h],
        )

    for b in range(2):
        for j in range(2):
            kv_load(b, j).start()
    for i in range(3):
        for h in range(heads):
            head_load(i, h).start()

    barrier = pltpu.get_barrier_semaphore()
    for off in range(1, chips):
        pl.semaphore_signal(barrier, inc=1, **to(lax.rem(chip + off, chips) * 2 + core))
    pl.semaphore_signal(barrier, inc=1, **to(mate))
    for b in range(2):
        for j in range(2):
            kv_load(b, j).wait()
    pl.semaphore_wait(barrier, chips)

    def hop(b, slot, j, target, sems):
        return pltpu.make_async_remote_copy(
            src_ref=kv.at[b, slot, j], dst_ref=kv.at[b, slot, j],
            send_sem=sems.at[b, slot, j], recv_sem=recv_sem.at[b, slot, j], **to(target),
        )

    def go_right(b, slot, j):
        return hop(b, slot, j, jnp.minimum(me + 2, n - 1), right_sem)

    def go_left(b, slot, j):
        return hop(b, slot, j, jnp.maximum(me - 2, 0), left_sem)

    def go_mate(b, slot, j):
        return hop(b, slot, j, mate, mate_sem)

    can_right = chip + 1 < chips
    can_left = chip > 0

    def spread_own(b):
        @pl.when(can_right)
        def _():
            for j in range(2):
                go_right(b, me, j).start()

        @pl.when(can_left)
        def _():
            for j in range(2):
                go_left(b, me, j).start()

        for j in range(2):
            go_mate(b, me, j).start()

    def relay(b, t):
        from_left = me - 2 * t
        from_right = me + 2 * t
        for j in range(2):
            @pl.when(chip - t >= 0)
            def _():
                slot = jnp.maximum(from_left, 0)
                hop(b, slot, j, mate, mate_sem).wait_recv()

                @pl.when(can_right)
                def _():
                    go_right(b, slot, j).start()
                go_mate(b, slot, j).start()

            @pl.when(chip + t < chips)
            def _():
                slot = jnp.minimum(from_right, n - 1)
                hop(b, slot, j, mate, mate_sem).wait_recv()

                @pl.when(can_left)
                def _():
                    go_left(b, slot, j).start()
                go_mate(b, slot, j).start()

    def take_mate(b, slot):
        for j in range(2):
            hop(b, slot, j, mate, mate_sem).wait_recv()

    spread_own(0)
    spread_own(1)

    lane = lax.broadcasted_iota(jnp.int32, (1, rows), 1) % tok
    mine = owner[me]
    places = jnp.where(lane < half, mine * half + lane, (2 * n - 1 - mine) * half + lane - half)
    key_row = lax.broadcasted_iota(jnp.int32, (half, rows), 0)

    def score_pair(b, d, queries):
        keys = kv[b, pl.ds(2 * d, 2), 0].reshape(2 * tok, dim)
        raw = dot_nt(keys, queries[...])
        best = top[...]
        for c in range(2):
            o = owner[2 * d + c]
            for part, slab in ((0, o), (1, 2 * n - 1 - o)):
                lo = c * tok + part * half
                piece = jnp.where(key_row <= places - slab * half, raw[lo:lo + half], LOW)
                scores[d, lo:lo + half] = piece
                best = jnp.maximum(best, groups(piece, jnp.maximum))
        top[...] = best

    def first_a(d):
        take_mate(0, 2 * d + 1 - core)
        score_pair(0, d, q_a)
        pgrad[d] = dot_nt(kv[0, pl.ds(2 * d, 2), 1].reshape(2 * tok, dim), g_a[...])

    for i in range(3):
        for h in range(heads):
            head_load(i, h).wait()
    top[...] = jnp.full_like(top, LOW)

    def gather_a(t, _):
        relay(0, t)

        @pl.when(chip - t + 1 >= 0)
        def _():
            first_a(jnp.maximum(chip - t + 1, 0))

        @pl.when(jnp.logical_and(chip + t - 1 < chips, t > 1))
        def _():
            first_a(jnp.minimum(chip + t - 1, chips - 1))

        @pl.when(t < chips - 1)
        def _():
            relay(1, t)
        return 0

    lax.fori_loop(1, chips, gather_a, 0)

    @pl.when(chip == chips - 1)
    def _():
        first_a(0)

    @pl.when(chip == 0)
    def _():
        first_a(chips - 1)

    relay(1, chips - 1)

    peak = jnp.max(top[...], axis=0, keepdims=True) * factor
    tot[...] = jnp.zeros_like(tot)
    dsum[...] = jnp.zeros_like(dsum)

    def second_a(i, _):
        p = jnp.exp2(scores[i] * factor - peak)
        scores[i] = p
        tot[...] += groups(p, jnp.add)
        dsum[...] += groups(p * pgrad[i], jnp.add)
        return 0

    lax.fori_loop(0, chips, second_a, 0)
    inv = 1.0 / jnp.sum(tot[...], axis=0, keepdims=True)
    delta = jnp.sum(dsum[...], axis=0, keepdims=True) * inv
    acc_t[...] = jnp.zeros_like(acc_t)

    def grads(d):
        prob = scores[d] * inv
        sg = (prob * (pgrad[d] - delta)).astype(BF16)
        both[0] = dot_nn(sg, q_a[...]).reshape(2, tok, dim)
        both[1] = dot_nn(prob.astype(BF16), g_a[...]).reshape(2, tok, dim)
        acc_t[...] += dot_tn(kv[0, pl.ds(2 * d, 2), 0].reshape(2 * tok, dim), sg)

    def pair(d):
        return pltpu.make_async_remote_copy(
            src_ref=pair_out.at[d], dst_ref=pair_in.at[d],
            send_sem=pair_send.at[d], recv_sem=pair_recv.at[d], **to(mate),
        )

    def far(d):
        return pltpu.make_async_remote_copy(
            src_ref=far_out.at[d], dst_ref=far_in.at[chip],
            send_sem=far_send.at[d], recv_sem=far_recv.at[chip], **to(d * 2 + core),
        )

    def ship(d):
        pair(d).wait_recv()
        far_out[d] = (own[d] + pair_in[d].astype(F32)).astype(BF16)
        far(d).start()

    def third_a(t, _):
        d = lax.rem(chip + t + 1, chips)
        grads(d)
        for j in range(2):
            pair_out[d, j] = both[j, 1 - core].astype(BF16)
        pair(d).start()
        for j in range(2):
            own[d, j] = both[j, core]

        @pl.when(t >= 1)
        def _():
            ship(lax.rem(chip + t, chips))
        return 0

    lax.fori_loop(0, chips, third_a, 0)

    def put(out, x):
        low = jnp.transpose(x).astype(BF16)
        for h in range(heads):
            out[:, h * dim:(h + 1) * dim] = low[h * tok:(h + 1) * tok]

    put(out_dq, acc_t[...] * scale)

    top[...] = jnp.full_like(top, LOW)

    def take_b(d, _):
        take_mate(1, 2 * d + 1 - core)
        return 0

    lax.fori_loop(0, chips, take_b, 0)

    def first_b(i, _):
        score_pair(1, i, q_b)
        return 0

    lax.fori_loop(0, chips, first_b, 0)
    peak_b = jnp.max(top[...], axis=0, keepdims=True) * factor
    tot[...] = jnp.zeros_like(tot)
    acc_t[...] = jnp.zeros_like(acc_t)

    def second_b(i, _):
        p = jnp.exp2(scores[i] * factor - peak_b)
        tot[...] += groups(p, jnp.add)
        acc_t[...] += dot_tn(kv[1, pl.ds(2 * i, 2), 1].reshape(2 * tok, dim), p.astype(BF16))
        return 0

    lax.fori_loop(0, chips, second_b, 0)
    total_b = jnp.sum(tot[...], axis=0, keepdims=True)
    put(out_b, acc_t[...] / total_b)

    pair(chip).wait_recv()
    own[chip] = own[chip] + pair_in[chip].astype(F32)

    def gather_sum(off, _):
        d = lax.rem(chip + off, chips)
        pltpu.make_async_remote_copy(
            src_ref=far_out.at[d], dst_ref=far_in.at[d],
            send_sem=far_send.at[d], recv_sem=far_recv.at[d], **to(d * 2 + core),
        ).wait_recv()
        own[chip] = own[chip] + far_in[d].astype(F32)
        return 0

    lax.fori_loop(1, chips, gather_sum, 0)
    out_dk[...] = (own[chip, 0] * scale).astype(BF16)
    out_dv[...] = own[chip, 1].astype(BF16)

    def drain_far(off, _):
        far(lax.rem(chip + off, chips)).wait_send()
        return 0

    lax.fori_loop(1, chips, drain_far, 0)

    def drain(d, _):
        pair(d).wait_send()
        slot = 2 * d + core
        for b in range(2):
            for j in range(2):
                go_mate(b, slot, j).wait_send()

                @pl.when(jnp.logical_and(can_right, d <= chip))
                def _():
                    go_right(b, slot, j).wait_send()

                @pl.when(jnp.logical_and(can_left, d >= chip))
                def _():
                    go_left(b, slot, j).wait_send()
        return 0

    lax.fori_loop(0, chips, drain, 0)


def emit(*refs):
    count = len(refs) // 2
    sems = refs[-1]
    copies = [
        pltpu.make_async_copy(refs[i], refs[count + i], sems.at[i]) for i in range(count)
    ]
    for copy in copies:
        copy.start()
    for copy in copies:
        copy.wait()


def on_device(n, qa, ka, va, ga, qb, kb, vb, owner):
    tok, dim = ka.shape
    heads = qa.shape[1] // dim
    rows = heads * tok
    chips = n // 2
    any_spec = pl.BlockSpec(memory_space=pl.ANY)
    sem = pltpu.SemaphoreType.DMA
    vmem_spec = pl.BlockSpec(memory_space=pltpu.VMEM)
    outs = pl.pallas_call(
        functools.partial(kernel, n, tok, heads, dim),
        out_shape=(
            pltpu.VMEM(qb.shape, BF16),
            pltpu.VMEM(qa.shape, BF16),
            pltpu.VMEM(ka.shape, BF16),
            pltpu.VMEM(va.shape, BF16),
        ),
        in_specs=[pl.BlockSpec(memory_space=pltpu.SMEM)] + [any_spec] * 7,
        out_specs=(vmem_spec,) * 4,
        scratch_shapes=[
            pltpu.VMEM((2, n, 2, tok, dim), BF16),
            pltpu.VMEM((rows, dim), BF16),
            pltpu.VMEM((rows, dim), BF16),
            pltpu.VMEM((rows, dim), BF16),
            pltpu.VMEM((chips, 2 * tok, rows), F32),
            pltpu.VMEM((chips, 2 * tok, rows), F32),
            pltpu.VMEM((8, rows), F32),
            pltpu.VMEM((8, rows), F32),
            pltpu.VMEM((8, rows), F32),
            pltpu.VMEM((dim, rows), F32),
            pltpu.VMEM((2, 2, tok, dim), F32),
            pltpu.VMEM((chips, 2, tok, dim), F32),
            pltpu.VMEM((chips, 2, tok, dim), BF16),
            pltpu.VMEM((chips, 2, tok, dim), BF16),
            pltpu.VMEM((chips, 2, tok, dim), BF16),
            pltpu.VMEM((chips, 2, tok, dim), BF16),
            sem((4 + 3 * heads,)),
            sem((2, n, 2)),
            sem((2, n, 2)),
            sem((2, n, 2)),
            sem((2, n, 2)),
            sem((chips,)),
            sem((chips,)),
            sem((chips,)),
            sem((chips,)),
        ],
        compiler_params=pltpu.CompilerParams(collective_id=0, has_side_effects=True),
    )(owner, qa, ka, va, ga, qb, kb, vb)
    return pl.pallas_call(
        emit,
        out_shape=tuple(jax.ShapeDtypeStruct(x.shape, x.dtype) for x in outs),
        in_specs=[vmem_spec] * 4,
        out_specs=(any_spec,) * 4,
        scratch_shapes=[sem((4,))],
        compiler_params=pltpu.CompilerParams(vmem_limit_bytes=8 * 2**20),
    )(*outs)


def solution(mesh):
    spec = P(("dp", "context"), "tensor")
    return jax.shard_map(
        functools.partial(on_device, mesh.shape["context"]),
        mesh=mesh,
        in_specs=(spec,) * 7 + (P(),),
        out_specs=(spec,) * 4,
        check_vma=False,
    )
```

```python
import functools

import jax
import jax.numpy as jnp
from jax import lax
from jax.experimental import pallas as pl
from jax.experimental.pallas import tpu as pltpu
from jax.sharding import PartitionSpec as P

LOW = -1e30
LOG2E = 1.4426950408889634
F32 = jnp.float32
BF16 = jnp.bfloat16


def dot_nt(a, b):
    return lax.dot_general(a, b, (((1,), (1,)), ((), ())), preferred_element_type=F32)


def dot_nn(a, b):
    return lax.dot_general(a, b, (((1,), (0,)), ((), ())), preferred_element_type=F32)


def dot_tn(a, b):
    return lax.dot_general(a, b, (((0,), (0,)), ((), ())), preferred_element_type=F32)


def groups(x, op):
    out = x[0:8]
    for i in range(8, x.shape[0], 8):
        out = op(out, x[i:i + 8])
    return out


def kernel(
    n, tok, heads, dim,
    owner, qa, ka, va, ga, qb, kb, vb,
    out_b, out_dq, out_dk, out_dv,
    kv, q_a, g_a, q_b, scores, pgrad, top, tot, dsum, acc_t, both,
    own, pair_out, pair_in, far_out, far_in,
    load_sem, recv_sem, right_sem, left_sem, mate_sem,
    pair_send, pair_recv, far_send, far_recv,
):
    chips = n // 2
    me = lax.axis_index("context")
    chip, core = me // 2, me % 2
    mate = chip * 2 + (1 - core)
    rows = heads * tok
    half = tok // 2
    scale = dim ** (-0.5)
    factor = scale * LOG2E

    def to(idx):
        return dict(device_id={"context": idx}, device_id_type=pl.DeviceIdType.MESH)

    def kv_load(b, j):
        src = ((ka, va), (kb, vb))[b][j]
        return pltpu.make_async_copy(src, kv.at[b, me, j], load_sem.at[b * 2 + j])

    def head_load(i, h):
        src, dst = ((qa, q_a), (ga, g_a), (qb, q_b))[i]
        return pltpu.make_async_copy(
            src.at[:, pl.ds(h * dim, dim)], dst.at[pl.ds(h * tok, tok), :],
            load_sem.at[4 + i * heads + h],
        )

    for b in range(2):
        for j in range(2):
            kv_load(b, j).start()
    for i in range(3):
        for h in range(heads):
            head_load(i, h).start()

    barrier = pltpu.get_barrier_semaphore()
    for off in range(1, chips):
        pl.semaphore_signal(barrier, inc=1, **to(lax.rem(chip + off, chips) * 2 + core))
    pl.semaphore_signal(barrier, inc=1, **to(mate))
    for b in range(2):
        for j in range(2):
            kv_load(b, j).wait()
    pl.semaphore_wait(barrier, chips)

    def hop(b, slot, j, target, sems):
        return pltpu.make_async_remote_copy(
            src_ref=kv.at[b, slot, j], dst_ref=kv.at[b, slot, j],
            send_sem=sems.at[b, slot, j], recv_sem=recv_sem.at[b, slot, j], **to(target),
        )

    def go_right(b, slot, j):
        return hop(b, slot, j, jnp.minimum(me + 2, n - 1), right_sem)

    def go_left(b, slot, j):
        return hop(b, slot, j, jnp.maximum(me - 2, 0), left_sem)

    def go_mate(b, slot, j):
        return hop(b, slot, j, mate, mate_sem)

    can_right = chip + 1 < chips
    can_left = chip > 0

    def spread_own(b):
        @pl.when(can_right)
        def _():
            for j in range(2):
                go_right(b, me, j).start()

        @pl.when(can_left)
        def _():
            for j in range(2):
                go_left(b, me, j).start()

        for j in range(2):
            go_mate(b, me, j).start()

    def relay(b, t):
        from_left = me - 2 * t
        from_right = me + 2 * t
        for j in range(2):
            @pl.when(chip - t >= 0)
            def _():
                slot = jnp.maximum(from_left, 0)
                hop(b, slot, j, mate, mate_sem).wait_recv()

                if b == 1:
                    @pl.when(can_right)
                    def _():
                        go_right(b, slot, j).start()
                go_mate(b, slot, j).start()

            @pl.when(chip + t < chips)
            def _():
                slot = jnp.minimum(from_right, n - 1)
                hop(b, slot, j, mate, mate_sem).wait_recv()

                if b == 1:
                    @pl.when(can_left)
                    def _():
                        go_left(b, slot, j).start()
                go_mate(b, slot, j).start()

    def take_mate(b, slot):
        for j in range(2):
            hop(b, slot, j, mate, mate_sem).wait_recv()

    def direct(d, j):
        return pltpu.make_async_remote_copy(
            src_ref=kv.at[0, me, j], dst_ref=kv.at[0, me, j],
            send_sem=right_sem.at[0, d, j], recv_sem=recv_sem.at[0, me, j], **to(2 * d + core),
        )

    for j in range(2):
        go_mate(0, me, j).start()
    for t in range(chips - 1, 0, -1):
        for j in range(2):
            @pl.when(chip + t < chips)
            def _():
                direct(jnp.minimum(chip + t, chips - 1), j).start()

            @pl.when(chip - t >= 0)
            def _():
                direct(jnp.maximum(chip - t, 0), j).start()
    spread_own(1)

    lane = lax.broadcasted_iota(jnp.int32, (1, rows), 1) % tok
    mine = owner[me]
    places = jnp.where(lane < half, mine * half + lane, (2 * n - 1 - mine) * half + lane - half)
    key_row = lax.broadcasted_iota(jnp.int32, (half, rows), 0)

    def score_pair(b, d, queries):
        keys = kv[b, pl.ds(2 * d, 2), 0].reshape(2 * tok, dim)
        raw = dot_nt(keys, queries[...])
        best = top[...]
        for c in range(2):
            o = owner[2 * d + c]
            for part, slab in ((0, o), (1, 2 * n - 1 - o)):
                lo = c * tok + part * half
                piece = jnp.where(key_row <= places - slab * half, raw[lo:lo + half], LOW)
                scores[d, lo:lo + half] = piece
                best = jnp.maximum(best, groups(piece, jnp.maximum))
        top[...] = best

    def first_a(d):
        take_mate(0, 2 * d + 1 - core)
        score_pair(0, d, q_a)
        pgrad[d] = dot_nt(kv[0, pl.ds(2 * d, 2), 1].reshape(2 * tok, dim), g_a[...])

    for i in range(3):
        for h in range(heads):
            head_load(i, h).wait()
    top[...] = jnp.full_like(top, LOW)

    def gather_a(t, _):
        relay(0, t)

        @pl.when(chip - t + 1 >= 0)
        def _():
            first_a(jnp.maximum(chip - t + 1, 0))

        @pl.when(jnp.logical_and(chip + t - 1 < chips, t > 1))
        def _():
            first_a(jnp.minimum(chip + t - 1, chips - 1))

        @pl.when(t < chips - 1)
        def _():
            relay(1, t)
        return 0

    lax.fori_loop(1, chips, gather_a, 0)

    @pl.when(chip == chips - 1)
    def _():
        first_a(0)

    @pl.when(chip == 0)
    def _():
        first_a(chips - 1)

    relay(1, chips - 1)

    peak = jnp.max(top[...], axis=0, keepdims=True) * factor
    tot[...] = jnp.zeros_like(tot)
    dsum[...] = jnp.zeros_like(dsum)

    def second_a(i, _):
        p = jnp.exp2(scores[i] * factor - peak)
        scores[i] = p
        tot[...] += groups(p, jnp.add)
        dsum[...] += groups(p * pgrad[i], jnp.add)
        return 0

    lax.fori_loop(0, chips, second_a, 0)
    inv = 1.0 / jnp.sum(tot[...], axis=0, keepdims=True)
    delta = jnp.sum(dsum[...], axis=0, keepdims=True) * inv
    acc_t[...] = jnp.zeros_like(acc_t)

    def grads(d):
        prob = scores[d] * inv
        sg = (prob * (pgrad[d] - delta)).astype(BF16)
        both[0] = dot_nn(sg, q_a[...]).reshape(2, tok, dim)
        both[1] = dot_nn(prob.astype(BF16), g_a[...]).reshape(2, tok, dim)
        acc_t[...] += dot_tn(kv[0, pl.ds(2 * d, 2), 0].reshape(2 * tok, dim), sg)

    def pair(d):
        return pltpu.make_async_remote_copy(
            src_ref=pair_out.at[d], dst_ref=pair_in.at[d],
            send_sem=pair_send.at[d], recv_sem=pair_recv.at[d], **to(mate),
        )

    def far(d):
        return pltpu.make_async_remote_copy(
            src_ref=far_out.at[d], dst_ref=far_in.at[chip],
            send_sem=far_send.at[d], recv_sem=far_recv.at[chip], **to(d * 2 + core),
        )

    def ship(d):
        pair(d).wait_recv()
        far_out[d] = (own[d] + pair_in[d].astype(F32)).astype(BF16)
        far(d).start()

    def third_a(t, _):
        d = lax.rem(chip + t + 1, chips)
        grads(d)
        for j in range(2):
            pair_out[d, j] = both[j, 1 - core].astype(BF16)
        pair(d).start()
        for j in range(2):
            own[d, j] = both[j, core]

        @pl.when(t >= 1)
        def _():
            ship(lax.rem(chip + t, chips))
        return 0

    lax.fori_loop(0, chips, third_a, 0)

    def put(out, x):
        low = jnp.transpose(x).astype(BF16)
        for h in range(heads):
            out[:, h * dim:(h + 1) * dim] = low[h * tok:(h + 1) * tok]

    put(out_dq, acc_t[...] * scale)

    top[...] = jnp.full_like(top, LOW)

    def take_b(d, _):
        take_mate(1, 2 * d + 1 - core)
        return 0

    lax.fori_loop(0, chips, take_b, 0)

    def first_b(i, _):
        score_pair(1, i, q_b)
        return 0

    lax.fori_loop(0, chips, first_b, 0)
    peak_b = jnp.max(top[...], axis=0, keepdims=True) * factor
    tot[...] = jnp.zeros_like(tot)
    acc_t[...] = jnp.zeros_like(acc_t)

    def second_b(i, _):
        p = jnp.exp2(scores[i] * factor - peak_b)
        tot[...] += groups(p, jnp.add)
        acc_t[...] += dot_tn(kv[1, pl.ds(2 * i, 2), 1].reshape(2 * tok, dim), p.astype(BF16))
        return 0

    lax.fori_loop(0, chips, second_b, 0)
    total_b = jnp.sum(tot[...], axis=0, keepdims=True)
    put(out_b, acc_t[...] / total_b)

    pair(chip).wait_recv()
    own[chip] = own[chip] + pair_in[chip].astype(F32)

    def gather_sum(off, _):
        d = lax.rem(chip + off, chips)
        pltpu.make_async_remote_copy(
            src_ref=far_out.at[d], dst_ref=far_in.at[d],
            send_sem=far_send.at[d], recv_sem=far_recv.at[d], **to(d * 2 + core),
        ).wait_recv()
        own[chip] = own[chip] + far_in[d].astype(F32)
        return 0

    lax.fori_loop(1, chips, gather_sum, 0)
    out_dk[...] = (own[chip, 0] * scale).astype(BF16)
    out_dv[...] = own[chip, 1].astype(BF16)

    def drain_far(off, _):
        far(lax.rem(chip + off, chips)).wait_send()
        return 0

    lax.fori_loop(1, chips, drain_far, 0)

    def drain(d, _):
        pair(d).wait_send()
        slot = 2 * d + core
        for b in range(2):
            for j in range(2):
                go_mate(b, slot, j).wait_send()
                if b == 0:
                    @pl.when(d != chip)
                    def _():
                        direct(d, j).wait_send()
                    continue

                @pl.when(jnp.logical_and(can_right, d <= chip))
                def _():
                    go_right(b, slot, j).wait_send()

                @pl.when(jnp.logical_and(can_left, d >= chip))
                def _():
                    go_left(b, slot, j).wait_send()
        return 0

    lax.fori_loop(0, chips, drain, 0)


def emit(*refs):
    count = len(refs) // 2
    sems = refs[-1]
    copies = [
        pltpu.make_async_copy(refs[i], refs[count + i], sems.at[i]) for i in range(count)
    ]
    for copy in copies:
        copy.start()
    for copy in copies:
        copy.wait()


def on_device(n, qa, ka, va, ga, qb, kb, vb, owner):
    tok, dim = ka.shape
    heads = qa.shape[1] // dim
    rows = heads * tok
    chips = n // 2
    any_spec = pl.BlockSpec(memory_space=pl.ANY)
    sem = pltpu.SemaphoreType.DMA
    vmem_spec = pl.BlockSpec(memory_space=pltpu.VMEM)
    outs = pl.pallas_call(
        functools.partial(kernel, n, tok, heads, dim),
        out_shape=(
            pltpu.VMEM(qb.shape, BF16),
            pltpu.VMEM(qa.shape, BF16),
            pltpu.VMEM(ka.shape, BF16),
            pltpu.VMEM(va.shape, BF16),
        ),
        in_specs=[pl.BlockSpec(memory_space=pltpu.SMEM)] + [any_spec] * 7,
        out_specs=(vmem_spec,) * 4,
        scratch_shapes=[
            pltpu.VMEM((2, n, 2, tok, dim), BF16),
            pltpu.VMEM((rows, dim), BF16),
            pltpu.VMEM((rows, dim), BF16),
            pltpu.VMEM((rows, dim), BF16),
            pltpu.VMEM((chips, 2 * tok, rows), F32),
            pltpu.VMEM((chips, 2 * tok, rows), F32),
            pltpu.VMEM((8, rows), F32),
            pltpu.VMEM((8, rows), F32),
            pltpu.VMEM((8, rows), F32),
            pltpu.VMEM((dim, rows), F32),
            pltpu.VMEM((2, 2, tok, dim), F32),
            pltpu.VMEM((chips, 2, tok, dim), F32),
            pltpu.VMEM((chips, 2, tok, dim), BF16),
            pltpu.VMEM((chips, 2, tok, dim), BF16),
            pltpu.VMEM((chips, 2, tok, dim), BF16),
            pltpu.VMEM((chips, 2, tok, dim), BF16),
            sem((4 + 3 * heads,)),
            sem((2, n, 2)),
            sem((2, n, 2)),
            sem((2, n, 2)),
            sem((2, n, 2)),
            sem((chips,)),
            sem((chips,)),
            sem((chips,)),
            sem((chips,)),
        ],
        compiler_params=pltpu.CompilerParams(collective_id=0, has_side_effects=True),
    )(owner, qa, ka, va, ga, qb, kb, vb)
    return pl.pallas_call(
        emit,
        out_shape=tuple(jax.ShapeDtypeStruct(x.shape, x.dtype) for x in outs),
        in_specs=[vmem_spec] * 4,
        out_specs=(any_spec,) * 4,
        scratch_shapes=[sem((4,))],
        compiler_params=pltpu.CompilerParams(vmem_limit_bytes=8 * 2**20),
    )(*outs)


def solution(mesh):
    spec = P(("dp", "context"), "tensor")
    return jax.shard_map(
        functools.partial(on_device, mesh.shape["context"]),
        mesh=mesh,
        in_specs=(spec,) * 7 + (P(),),
        out_specs=(spec,) * 4,
        check_vma=False,
    )
```
